32 devices in a mesh: dp: 8 (over z, x), mp: 4 (over y, core).
Axes of the slice: x: 2, y: 2, z: 4, core: 2. Of those that a mesh axis runs over, the one named last changes fastest.
Arguments:
- tokens: bfloat16 [1024, 4096], P('dp'), may hold values from -6 to 6
- cotangent: bfloat16 [1024, 4096], P('dp', 'mp'), may hold values from -6 to 6
- sketch: float32 [4096, 128], P('dp'), may hold values from -12 to 12
Outputs:
- precond: bfloat16 [4096, 4096], P('dp', 'mp')
- new_sketch: float32 [4096, 128], P('dp')
The draws below stay inside these ranges and needn't reach their ends.
All inputs are finite; a program needn't handle non-finite values.
Results may differ from the reference program's by a relative error of at most 0.001.
Values sent between devices are 32-bit elements; how exact they have to be, the bound alone decides.
No kernel may reach another device: no remote copies, remote signals or barrier semaphores. Data moves between devices by JAX's collectives and lax.ppermute only.
A program may use at most 64 MiB of HBM per device.

```python
import math
import jax
import jax.numpy as jnp
from jax import lax

D = 4096
COLS = 4096
RANK = 128
ITERS = 1
TOKENS = 1024


def strengthened(entries, stream_key, source, target, blocks, factor):
    owner, partner = [(jnp.arange(entries.shape[position]) // (entries.shape[position] // blocks)).reshape([-1 if axis == position else 1 for axis in range(entries.ndim)]) for position in (source, target)]
    chosen = jax.random.permutation(stream_key, blocks)[partner]
    strong = (owner == chosen) | (owner == (partner + blocks // 2) % blocks)
    return jnp.where(strong, factor * entries, entries)


def shard_levels(stream_key, dims, pieces, least, top_value):
    factor_of = 1.0
    for dim, shards_of in pieces:
        steps = jax.random.uniform(jax.random.fold_in(jax.random.fold_in(stream_key, 6), dim), (shards_of,), jnp.float32, least / len(pieces), top_value / len(pieces))
        factor_of = factor_of * jnp.repeat(jnp.exp(steps), dims[dim] // shards_of).reshape((-1,) + (1,) * (len(dims) - 1 - dim))
    return factor_of


def gaussian(rng, dims, deviation, most, pieces=(), kind=jnp.bfloat16):
    factor_of = shard_levels(rng, dims, pieces, -0.22, 0.18) if pieces else 1.0
    array = jax.random.normal(rng, dims, jnp.float32) * deviation * factor_of
    return jnp.minimum(jnp.maximum(array, -most), most).astype(kind)


def bell_draw_with(stream_key, dims, scale, bound, pieces, heavy, held_as=jnp.bfloat16):
    entries = scale * jax.random.normal(stream_key, dims, jnp.float32)
    if pieces:
        entries = entries * shard_levels(stream_key, dims, pieces, -0.22, 0.18)
    return jnp.clip(strengthened(entries, jax.random.fold_in(stream_key, 3), *heavy), -bound, bound).astype(held_as)


def setup_inputs(seed: int = 0) -> dict:
    streams_of = jax.random.split(jax.random.key(seed), 4)
    return {
        "tokens": bell_draw_with(streams_of[0], (TOKENS, D), 1.0, 6.0, ((0, 8),), (0, 1, 8, 2.0)),
        "cotangent": gaussian(streams_of[1], (TOKENS, COLS), 1.0, 6.0, ((0, 8), (1, 4))),
        "sketch": gaussian(streams_of[2], (D, RANK), 2.0, 12.0, ((0, 8),), jnp.float32),
    }


DECAY_RATE = 0.9
RIDGE_FRAC = 0.0001

def product(left_mat, right_mat):
    return jnp.dot(left_mat, right_mat, precision=lax.Precision.HIGHEST)

def right_solve(values, lower_tri):
    return lax.linalg.triangular_solve(lower_tri, values, left_side=False, lower=True, transpose_a=True)

def left_solve(lower_tri, values, transpose):
    return lax.linalg.triangular_solve(lower_tri, values, left_side=True, lower=True, transpose_a=transpose)

def spd_solve(matrix, target):
    lower_tri = jnp.linalg.cholesky(matrix)
    return left_solve(lower_tri, left_solve(lower_tri, target, False), True)

def reference(tokens, cotangent, sketch):
    gradient = jnp.dot(tokens.T.astype(jnp.float32), cotangent.astype(jnp.float32), preferred_element_type=jnp.float32) * (1.0 / math.sqrt(TOKENS))

    def covariance(basis_now):
        return DECAY_RATE * product(sketch, product(sketch.T, basis_now)) + product(gradient, product(gradient.T, basis_now))
    basis_now = sketch
    for iteration in range(ITERS):
        applied = covariance(basis_now)
        basis_now = right_solve(applied, jnp.linalg.cholesky(product(applied.T, applied)))
    applied = covariance(basis_now)
    rayleigh = product(basis_now.T, applied)
    rayleigh = 0.5 * (rayleigh + rayleigh.T)
    mean_level = jnp.trace(rayleigh) / RANK
    identity = jnp.eye(RANK, dtype=jnp.float32)
    new_sketch = right_solve(applied, jnp.linalg.cholesky(rayleigh + RIDGE_FRAC * mean_level * identity))
    inner_mat = mean_level * identity + product(new_sketch.T, new_sketch)
    coeffs = spd_solve(inner_mat, product(new_sketch.T, gradient))
    precond = gradient - product(new_sketch, coeffs)
    return (precond.astype(jnp.bfloat16), new_sketch)
```

```python
import math

import jax
import jax.numpy as jnp
from jax import lax
from jax.experimental import pallas as pl
from jax.experimental.pallas import tpu as pltpu
from jax.sharding import PartitionSpec as P

DECAY_RATE = 0.9
RIDGE_FRAC = 0.0001
SUBLANES = 8


def product(left_mat, right_mat):
    return jnp.dot(left_mat, right_mat, precision=lax.Precision.HIGHEST)


def right_solve(values, lower_tri):
    return lax.linalg.triangular_solve(
        lower_tri, values, left_side=False, lower=True, transpose_a=True
    )


def left_solve(lower_tri, values, transpose):
    return lax.linalg.triangular_solve(
        lower_tri, values, left_side=True, lower=True, transpose_a=transpose
    )


def spd_solve(matrix, target):
    lower_tri = jnp.linalg.cholesky(matrix)
    return left_solve(lower_tri, left_solve(lower_tri, target, False), True)


def feature_shards(tokens, cotangent, sketch):
    dp_count = lax.axis_size("dp")
    rank_size = sketch.shape[1]
    norm_scale = 1.0 / math.sqrt(tokens.shape[0] * dp_count)
    gradient = lax.psum_scatter(
        lax.dot_general(
            tokens, cotangent, (((0,), (0,)), ((), ())), preferred_element_type=jnp.float32
        )
        * norm_scale,
        "dp",
        scatter_dimension=0,
        tiled=True,
    )
    identity = jnp.eye(rank_size, dtype=jnp.float32)

    def covariance(sketch_proj, grad_proj):
        partial_cols = product(gradient, grad_proj)
        summed = lax.psum(partial_cols, "mp")
        return DECAY_RATE * product(sketch, sketch_proj) + summed

    sketch_proj, grad_proj = lax.psum(
        (product(sketch.T, sketch), product(gradient.T, sketch)), "dp"
    )
    applied = covariance(sketch_proj, grad_proj)
    gram_mat, sketch_image, grad_image = lax.psum(
        (product(applied.T, applied), product(sketch.T, applied), product(gradient.T, applied)),
        "dp",
    )
    previous_low = jnp.linalg.cholesky(gram_mat)
    previous = applied
    applied = covariance(
        right_solve(sketch_image, previous_low), right_solve(grad_image, previous_low)
    )
    cross_prev, self_image, image_grad = lax.psum(
        (product(previous.T, applied), product(applied.T, applied), product(applied.T, gradient)),
        "dp",
    )
    rayleigh = left_solve(previous_low, cross_prev, False)
    rayleigh = 0.5 * (rayleigh + rayleigh.T)
    mean_level = jnp.trace(rayleigh) / rank_size
    new_low = jnp.linalg.cholesky(rayleigh + RIDGE_FRAC * mean_level * identity)
    new_sketch = right_solve(applied, new_low)
    self_gram = right_solve(left_solve(new_low, self_image, False), new_low)
    cross_mat = left_solve(new_low, image_grad, False)
    inner_mat = mean_level * identity + self_gram
    precond = gradient - product(new_sketch, spd_solve(inner_mat, cross_mat))
    return (precond.astype(jnp.bfloat16), new_sketch)


def swap(values, axis, bit):
    pairs = [(device, device ^ bit) for device in range(lax.axis_size(axis))]
    return lax.ppermute(values, axis, pairs)


def bits_of(count):
    return [1 << step for step in range(count.bit_length() - 1)]


def halves(values, axis, bit):
    half = values.shape[0] // 2
    side = (lax.axis_index(axis) // bit) % 2
    kept = lax.dynamic_slice_in_dim(values, side * half, half, 0)
    sent = lax.dynamic_slice_in_dim(values, (1 - side) * half, half, 0)
    return kept, sent


def joined(kept, axis, bit, dim=0):
    side = (lax.axis_index(axis) // bit) % 2
    other = swap(kept, axis, bit)
    low = jnp.where(side == 0, kept, other)
    high = jnp.where(side == 0, other, kept)
    return jnp.concatenate([low, high], dim)


def sum_all(values):
    for bit in bits_of(lax.axis_size("mp")):
        kept, sent = halves(values, "mp", bit)
        values = kept + swap(sent, "mp", bit)
    for bit in bits_of(lax.axis_size("dp")):
        values = values + swap(values, "dp", bit)
    for bit in reversed(bits_of(lax.axis_size("mp"))):
        values = joined(values, "mp", bit)
    return values


def sum_mp(values):
    first, *others = bits_of(lax.axis_size("mp"))
    kept, sent = halves(values, "mp", first)
    values = kept + swap(sent, "mp", first)
    for bit in others:
        values = values + swap(values, "mp", bit)
    return joined(values, "mp", first)


def cycle_of(count):
    return [2 * row for row in range(count // 2)] + [
        2 * row + 1 for row in reversed(range(count // 2))
    ]


def gather_dp(block):
    count = lax.axis_size("dp")
    order = cycle_of(count)
    place = [order.index(device) for device in range(count)]
    here = jnp.asarray(place, jnp.int32)[lax.axis_index("dp")]
    walk = jnp.asarray(order, jnp.int32)
    ahead = [(order[step], order[(step + 1) % count]) for step in range(count)]
    back = [(target, source) for source, target in ahead]
    wide = block.astype(jnp.float32)
    half = block.shape[0] // 2
    size = block.shape[0]
    arrived, rows = [wide], [lax.axis_index("dp") * size]
    from_back, from_ahead = wide, wide
    for step in range(1, count // 2):
        from_back = lax.ppermute(from_back, "dp", ahead)
        from_ahead = lax.ppermute(from_ahead, "dp", back)
        arrived += [from_back, from_ahead]
        rows += [walk[(here - step) % count] * size, walk[(here + step) % count] * size]
    far = walk[(here + count // 2) % count] * size
    arrived.append(lax.ppermute(from_back[:half], "dp", ahead))
    arrived.append(lax.ppermute(from_ahead[half:], "dp", back))
    rows += [far, far + half]
    return placed(jnp.stack(rows), arrived, (count * size,) + block.shape[1:])


def place_kernel(rows_ref, *refs):
    *block_refs, whole_ref = refs
    for index, block_ref in enumerate(block_refs):
        size = block_ref.shape[0]
        row = pl.multiple_of(rows_ref[index], size)
        whole_ref[pl.ds(row, size), :] = block_ref[...].astype(jnp.bfloat16)


def placed(rows, blocks, shape):
    return pl.pallas_call(
        place_kernel,
        out_shape=jax.ShapeDtypeStruct(shape, jnp.bfloat16),
        in_specs=[pl.BlockSpec(memory_space=pltpu.SMEM)]
        + [pl.BlockSpec(memory_space=pltpu.VMEM)] * len(blocks),
        out_specs=pl.BlockSpec(memory_space=pltpu.VMEM),
        name="place",
    )(rows, *blocks)


def narrowed(block):
    return placed(jnp.zeros((1,), jnp.int32), [block], block.shape)


def pieces(values):
    high = lax.reduce_precision(values, 8, 7)
    rest = values - high
    middle = lax.reduce_precision(rest, 8, 7)
    parts = (high, middle, rest - middle)
    return jnp.concatenate([part.astype(jnp.bfloat16) for part in parts], -1)


def exact_dot(left, right, dim):
    wide = lax.dot_general(
        left, pieces(right), (((dim,), (0,)), ((), ())), preferred_element_type=jnp.float32
    )
    count = right.shape[1]
    return wide[:, :count] + wide[:, count : 2 * count] + wide[:, 2 * count :]


def factor_kernel(matrix_ref, lower_inv_ref):
    batch, size, _ = matrix_ref.shape
    row_ids = lax.broadcasted_iota(jnp.int32, (SUBLANES, 2 * size), 0)
    lanes = lax.broadcasted_iota(jnp.int32, (SUBLANES, size), 1)
    subs = lax.broadcasted_iota(jnp.int32, (SUBLANES, size), 0)
    panels = []
    for item in range(batch):
        rows = []
        for start in range(0, size, SUBLANES):
            eye = (lanes == subs + start).astype(jnp.float32)
            rows.append(
                jnp.concatenate([matrix_ref[item, pl.ds(start, SUBLANES), :], eye], 1)
            )
        panels.append(rows)
    count = size // SUBLANES
    for panel in range(count):
        for step in range(SUBLANES):
            pivot_lane = panel * SUBLANES + step
            for item in range(batch):
                rows = panels[item]
                here = rows[panel]
                pivot = here[step : step + 1, pivot_lane : pivot_lane + 1]
                root = lax.rsqrt(pivot)
                root = root * (1.5 - 0.5 * pivot * root * root)
                row = here[step : step + 1, :] * root
                column = here[:, pivot_lane : pivot_lane + 1] * root
                here = jnp.where(
                    row_ids == step, row, jnp.where(row_ids > step, here - column * row, here)
                )
                rows[panel] = here
                for later in range(panel + 1, count):
                    column = rows[later][:, pivot_lane : pivot_lane + 1] * root
                    rows[later] = rows[later] - column * row
    for item in range(batch):
        for panel in range(count):
            lower_inv_ref[item, pl.ds(panel * SUBLANES, SUBLANES), :] = panels[item][panel][
                :, size:
            ]


def inverse_factors(matrices):
    return pl.pallas_call(
        factor_kernel,
        out_shape=jax.ShapeDtypeStruct(matrices.shape, jnp.float32),
        in_specs=[pl.BlockSpec(memory_space=pltpu.VMEM)],
        out_specs=pl.BlockSpec(memory_space=pltpu.VMEM),
        name="factor",
    )(matrices)


def token_shards(tokens, cotangent, sketch):
    dp_count, mp_count = lax.axis_size("dp"), lax.axis_size("mp")
    here, features = tokens.shape
    rank_size = sketch.shape[1]
    total = here * dp_count
    own = sketch.shape[0]
    part = own // mp_count
    mp_index = lax.axis_index("mp")
    identity = jnp.eye(rank_size, dtype=jnp.float32)

    grads = gather_dp(cotangent)

    cut = lax.dynamic_index_in_dim(
        tokens.reshape(here, dp_count, mp_count, part), mp_index, 2, keepdims=False
    )
    cut = jnp.swapaxes(cut, 0, 1).astype(jnp.float32)
    cut = lax.all_to_all(cut, "dp", 0, 0, tiled=True).reshape(total, part)
    narrow = narrowed(cut)
    sketch_part = lax.dynamic_slice_in_dim(sketch, mp_index * part, part, 0)
    first = sum_all(
        jnp.concatenate(
            [exact_dot(narrow, sketch_part, 1), product(sketch_part.T, sketch_part)], 0
        )
    )
    start, sketch_gram = first[:total], first[total:]

    wide = cut
    for bit in reversed(bits_of(mp_count)):
        wide = joined(wide, "mp", bit, 1)
    turned = [0]
    for bit in reversed(bits_of(mp_count)):
        turned = turned + [index + bit for index in turned]
    wide = jnp.concatenate(
        [lax.slice_in_dim(wide, turned.index(j) * part, (turned.index(j) + 1) * part, axis=1) for j in range(mp_count)],
        1,
    )
    own_tokens = narrowed(wide)

    def spread(image):
        columns = exact_dot(grads, image, 0) * (1.0 / total)
        coefs = exact_dot(grads, columns, 1)
        return coefs, exact_dot(own_tokens, exact_dot(own_tokens, coefs, 0), 1)

    coefs, image = spread(start)
    image = sum_all(image) + DECAY_RATE * product(start, sketch_gram)
    next_coefs, next_image = spread(image)

    coefs = sum_mp(coefs)
    sketch_coefs = DECAY_RATE * sketch_gram
    sketch_image = product(sketch_gram, sketch_coefs) + product(start.T, coefs)
    gram_mat = product(sketch_coefs.T, sketch_image) + product(coefs.T, image)
    low_inv = inverse_factors(gram_mat[None])[0]

    next_sketch_coefs = DECAY_RATE * sketch_image
    next_image = sum_all(next_image) + product(start, next_sketch_coefs)
    next_coefs = sum_mp(next_coefs)

    next_image = product(next_image, low_inv.T)
    next_coefs = product(next_coefs, low_inv.T)
    next_sketch_coefs = product(next_sketch_coefs, low_inv.T)
    next_sketch_image = product(sketch_gram, next_sketch_coefs) + product(start.T, next_coefs)
    cross_prev = product(sketch_coefs.T, next_sketch_image) + product(coefs.T, next_image)
    self_image = product(next_sketch_coefs.T, next_sketch_image) + product(
        next_coefs.T, next_image
    )
    rayleigh = product(low_inv, cross_prev)
    rayleigh = 0.5 * (rayleigh + rayleigh.T)
    mean_level = jnp.trace(rayleigh) / rank_size
    ridged = rayleigh + RIDGE_FRAC * mean_level * identity
    inner_mat = mean_level * ridged + 0.5 * (self_image + self_image.T)
    new_inv, inner_inv = inverse_factors(jnp.stack([ridged, inner_mat]))

    applied = product(sketch, next_sketch_coefs) + exact_dot(own_tokens, next_coefs, 0)
    new_sketch = product(applied, new_inv.T)
    norm_scale = 1.0 / math.sqrt(total)
    image_grad = exact_dot(grads, next_image, 0).T * norm_scale
    coeffs = product(inner_inv.T, product(inner_inv, image_grad))
    gradient = norm_scale * lax.dot_general(
        own_tokens, grads, (((0,), (0,)), ((), ())), preferred_element_type=jnp.float32
    )
    precond = gradient - product(applied, coeffs)
    return (precond.astype(jnp.bfloat16), new_sketch)


def power_of_two(count):
    return count > 1 and count & (count - 1) == 0


def shards(tokens, cotangent, sketch):
    dp_count, mp_count = lax.axis_size("dp"), lax.axis_size("mp")
    tile = mp_count * SUBLANES
    fits = (
        tokens.shape[0] * dp_count < tokens.shape[1]
        and power_of_two(dp_count)
        and power_of_two(mp_count)
        and dp_count > 2
        and sketch.shape[0] % (mp_count * SUBLANES) == 0
        and sketch.shape[1] % tile == 0
        and tokens.shape[0] % tile == 0
    )
    body = token_shards if fits else feature_shards
    return body(tokens, cotangent, sketch)


def solution(mesh):
    in_specs = (P("dp", None), P("dp", "mp"), P("dp", None))
    out_specs = (P("dp", "mp"), P("dp", None))
    return jax.shard_map(shards, mesh=mesh, in_specs=in_specs, out_specs=out_specs, check_vma=False)
```
